32 devices in a mesh: mesh: 8 (over y, x, core), harm: 4 (over z).
Axes of the slice: x: 2, y: 2, z: 4, core: 2. Of those that a mesh axis runs over, the one named last changes fastest.
Arguments:
- field_in: float32 [64, 40960], P('harm', 'mesh'), may hold values from -6 to 6
- faces: int32 [2, 8192], P(None, 'mesh'), may hold values from 0 to 5119, as said below
- connectivity: int32 [6, 32768], P(None, 'mesh'), may hold values from 0 to 7167
- curl_vectors: float32 [3, 6, 32768], P(None, None, 'mesh'), may hold values from -2.4 to 2.4
- operating_point: float32 [64, 3, 8, 4096], P(None, None, None, ('mesh', 'harm')), may hold values from -2.5 to 2.5
- material: int32 [8, 4096], P(None, ('mesh', 'harm')), may hold values from 0 to 3
- bh_knots: int32 [8], replicated, may hold values from 0 to 15
- curve_base: float32 [4], replicated, may hold values from 0.5 to 2
- curve_slopes: float32 [4, 8], replicated, may hold values from 0.02 to 0.2
Outputs:
- product: float32 [64, 40960], P('harm', 'mesh')
The draws below stay inside these ranges and needn't reach their ends.
Inputs may be any that keep to these rules, and one draw needn't show every extreme that they name: `faces`: for each partition the 1024 lower face edges and the 1024 upper face edges are 2048 distinct local edge numbers. `connectivity`: numbers below 5120 are the partition's own edges, the next 1024 the ghost edges after the upper face list of the partition below, the last 1024 those after the lower face list of the partition above.
All inputs are finite; a program needn't handle non-finite values.
Results may differ from the reference program's by a relative error of at most 0.0003.
Values sent between devices are 32-bit elements; how exact they have to be, the bound alone decides.
No kernel may reach another device: no remote copies, remote signals or barrier semaphores. Data moves between devices by JAX's collectives and lax.ppermute only.
A program may use at most 128 MiB of HBM per device.

```python
import math
import jax
import jax.numpy as jnp
from jax import lax

SAMPLES = 64
E_PART = 4096
KNOTS = 8
MATERIALS = 4
EDGES_PART = 5120
FACE = 1024
ELEMS = 32768
EDGES = 40960
N_MESH = 8


def draw_faces(key, part):
    keys = jax.random.split(jax.random.fold_in(key, 7), N_MESH)

    def single(sub_key):
        order = jax.random.permutation(sub_key, jnp.arange(EDGES_PART, dtype=jnp.int32))
        return order[:2 * FACE].reshape(2, FACE)
    lists = jax.vmap(single)(keys)
    return jnp.transpose(lists, (1, 0, 2)).reshape(2, N_MESH * FACE).astype(jnp.int32)


def set_ends(values, rng, smallest, largest):
    place = [jax.random.randint(jax.random.fold_in(rng, axis), (), 0, length) for axis, length in enumerate(values.shape)]
    longest = values.shape.index(max(values.shape))
    next_to = place[:longest] + [(place[longest] + 1) % values.shape[longest]] + place[longest + 1:]
    return values.at[tuple(place)].set(smallest).at[tuple(next_to)].set(largest)


def block_levels(rng, extent, cuts, smallest, high):
    def one(axis_at, shards_of):
        heights = jax.random.uniform(jax.random.fold_in(jax.random.fold_in(rng, 6), axis_at), (shards_of,), jnp.float32, smallest / len(cuts), high / len(cuts))
        return jnp.repeat(jnp.exp(heights), extent[axis_at] // shards_of).reshape((-1,) + (1,) * (len(extent) - axis_at - 1))

    factor_of = one(*cuts[0])
    for cut in cuts[1:]:
        factor_of = factor_of * one(*cut)
    return factor_of


def noise(stream_key, dims, scale, most, shards=(), kind=jnp.bfloat16):
    drawn = scale * jax.random.normal(stream_key, dims, jnp.float32)
    if shards:
        drawn = drawn * block_levels(stream_key, dims, shards, -0.22, 0.18)
    return jnp.clip(drawn, -most, most).astype(kind)


def setup_inputs(seed: int = 0) -> dict:
    key_of = jax.random.split(jax.random.key(seed), 10)
    return {
        "field_in": noise(key_of[0], (SAMPLES, EDGES), 1.0, 6.0, ((0, 4), (1, 8)), jnp.float32),
        "faces": draw_faces(jax.random.fold_in(key_of[9], 71), 0),
        "connectivity": set_ends(jax.random.randint(key_of[2], (6, ELEMS), 0, EDGES_PART + 2 * FACE), jax.random.fold_in(key_of[2], 1), 0, (EDGES_PART + 2 * FACE) - 1).astype(jnp.int32),
        "curl_vectors": noise(key_of[3], (3, 6, ELEMS), 0.4, 2.4, ((2, 8),), jnp.float32),
        "operating_point": noise(key_of[4], (SAMPLES, 3, N_MESH, E_PART), 0.7, 2.5, ((3, 32),), jnp.float32),
        "material": set_ends(jax.random.randint(key_of[5], (N_MESH, E_PART), 0, MATERIALS), jax.random.fold_in(key_of[5], 1), 0, MATERIALS - 1).astype(jnp.int32),
        "bh_knots": set_ends(jax.random.randint(key_of[6], (KNOTS,), 0, 16), jax.random.fold_in(key_of[6], 1), 0, 15).astype(jnp.int32),
        "curve_base": jnp.clip(jnp.exp(jax.random.uniform(key_of[7], (MATERIALS,), jnp.float32, math.log(0.5), math.log(2.0))), 0.5, 2.0),
        "curve_slopes": jnp.clip(jnp.exp(jax.random.uniform(key_of[8], (MATERIALS, KNOTS), jnp.float32, math.log(0.02), math.log(0.2))), 0.02, 0.2),
    }


KNOT_STEP = 0.25
KNOT_WIDTH = 0.5


def dft_tables(length):
    sample_idx = jnp.arange(length, dtype=jnp.int32)
    coef_idx = jnp.arange(length, dtype=jnp.int32)
    half_len = length // 2
    harmonic = jnp.where(coef_idx < half_len, coef_idx, coef_idx - half_len + 1)
    harmonic = jnp.where(coef_idx == length - 1, half_len, harmonic)
    is_sine = (coef_idx >= half_len) & (coef_idx < length - 1)
    phase_int = (harmonic[:, None] * sample_idx[None, :]) % length
    angles = phase_int.astype(jnp.float32) * (2.0 * jnp.pi / length)
    basis_rows = jnp.where(is_sine[:, None], jnp.sin(angles), jnp.cos(angles))
    weight = jnp.where((coef_idx == 0) | (coef_idx == length - 1), 1.0 / length, 2.0 / length)
    return basis_rows.T, basis_rows * weight[:, None].astype(jnp.float32)


def apply_tensor(flux_step, point, material, bh_knots, curve_base, curve_slopes):
    kind_ids = jnp.arange(curve_base.shape[0], dtype=jnp.int32).reshape((-1,) + (1,) * material.ndim)
    one_hot = (material[None] == kind_ids).astype(jnp.float32)
    base_elem = jnp.einsum('a,a...->...', curve_base, one_hot, precision=lax.Precision.HIGHEST)
    slope_elem = jnp.einsum('ak,a...->k...', curve_slopes, one_hot, precision=lax.Precision.HIGHEST)
    flux_sq = jnp.sum(point * point, axis=1)
    knot_pos = bh_knots.astype(jnp.float32) * KNOT_STEP
    scaled = (flux_sq[None] - knot_pos.reshape((-1,) + (1,) * flux_sq.ndim)) / KNOT_WIDTH
    reluct = base_elem[None] + jnp.sum(slope_elem[:, None] * jax.nn.softplus(scaled), axis=0)
    slope_sum = jnp.sum(slope_elem[:, None] * jax.nn.sigmoid(scaled), axis=0) / KNOT_WIDTH
    projected = jnp.sum(point * flux_step, axis=1)
    return reluct[:, None] * flux_step + 2.0 * (slope_sum * projected)[:, None] * point


def reference(field_in, faces, connectivity, curl_vectors, operating_point, material, bh_knots, curve_base, curve_slopes):
    owned = field_in.reshape(SAMPLES, N_MESH, EDGES_PART)
    face_ids = faces.reshape(2, N_MESH, FACE)
    lower_face = jnp.take_along_axis(owned, face_ids[0][None], axis=2)
    upper_face = jnp.take_along_axis(owned, face_ids[1][None], axis=2)
    extended = jnp.concatenate([owned, jnp.roll(upper_face, 1, axis=1), jnp.roll(lower_face, -1, axis=1)], axis=2)
    inverse, forward = dft_tables(SAMPLES)

    def partition(inputs):
        ext_part, conn_part, curl_part, point_part, mat_part = inputs
        gathered = ext_part[:, conn_part]
        flux_coef = jnp.einsum('ije,cje->cie', curl_part, gathered, precision=lax.Precision.HIGHEST)
        flux_step = jnp.einsum('tc,cie->tie', inverse, flux_coef, precision=lax.Precision.HIGHEST)
        field_step = apply_tensor(flux_step, point_part, mat_part, bh_knots, curve_base, curve_slopes)
        field_coef = jnp.einsum('ct,tie->cie', forward, field_step, precision=lax.Precision.HIGHEST)
        contrib = jnp.einsum('ije,cie->cje', curl_part, field_coef, precision=lax.Precision.HIGHEST)
        zeros_ext = jnp.zeros((SAMPLES, EDGES_PART + 2 * FACE), jnp.float32)
        return zeros_ext.at[:, conn_part.reshape(-1)].add(contrib.reshape(SAMPLES, -1))

    assembled = lax.map(partition, (
        jnp.moveaxis(extended, 1, 0),
        jnp.moveaxis(connectivity.reshape(6, N_MESH, E_PART), 1, 0),
        jnp.moveaxis(curl_vectors.reshape(3, 6, N_MESH, E_PART), 2, 0),
        jnp.moveaxis(operating_point, 2, 0),
        material))
    own_sums = assembled[:, :, :EDGES_PART]
    from_below = jnp.roll(assembled[:, :, EDGES_PART + FACE:], 1, axis=0)
    from_above = jnp.roll(assembled[:, :, EDGES_PART:EDGES_PART + FACE], -1, axis=0)

    def add_faces(sums, lower_ids, upper_ids, below_part, above_part):
        return sums.at[:, lower_ids].add(below_part).at[:, upper_ids].add(above_part)

    result = jax.vmap(add_faces)(own_sums, face_ids[0], face_ids[1], from_below, from_above)
    return jnp.moveaxis(result, 0, 1).reshape(SAMPLES, N_MESH * EDGES_PART)
```

```python
import functools

import jax
import jax.numpy as jnp
import numpy as np
from jax import lax
from jax.experimental import pallas as pl
from jax.experimental.pallas import tpu as pltpu
from jax.sharding import PartitionSpec as P

KNOT_STEP = 0.25
KNOT_WIDTH = 0.5
WIDE = 256
SHIFT = 8
BF = jnp.bfloat16
F32 = jnp.float32
VM = pl.BlockSpec(memory_space=pltpu.VMEM)
SM = pl.BlockSpec(memory_space=pltpu.SMEM)
NT = (((1,), (1,)), ((), ()))


def dft_tables(length):
    coef = np.arange(length)
    half = length // 2
    harmonic = np.where(coef < half, coef, coef - half + 1)
    harmonic = np.where(coef == length - 1, half, harmonic)
    is_sine = (coef >= half) & (coef < length - 1)
    angles = (harmonic[:, None] * coef[None, :] % length) * (2.0 * np.pi / length)
    rows = np.where(is_sine[:, None], np.sin(angles), np.cos(angles))
    weight = np.where((coef == 0) | (coef == length - 1), 1.0 / length, 2.0 / length)
    return rows.T.astype(np.float32), (rows * weight[:, None]).astype(np.float32)


def split(value):
    high = value.astype(BF)
    return high, (value - high.astype(F32)).astype(BF)


def cost(flops):
    return pl.CostEstimate(flops=flops, bytes_accessed=4 << 20, transcendentals=0)


def fill_tiles(source_ref, tiles):
    rows, columns = source_ref.shape
    for tile in range(columns // WIDE):
        high, low = split(source_ref[:, tile * WIDE : (tile + 1) * WIDE])
        tiles[tile * rows : (tile + 1) * rows, :WIDE] = high
        tiles[tile * rows : (tile + 1) * rows, WIDE:] = low


def one_hot(ids, iota):
    low = jnp.bitwise_and(ids, WIDE - 1)
    return (jnp.broadcast_to(low, iota.shape) == iota).astype(F32).astype(BF)


def pick(tiles, ids, iota, rows, first):
    hot = one_hot(ids, iota)
    table = jnp.dot(tiles[:, :WIDE], hot, preferred_element_type=F32)
    table = table + jnp.dot(tiles[:, WIDE:], hot, preferred_element_type=F32)
    tile_of = jnp.broadcast_to(jnp.right_shift(ids, SHIFT), (rows, ids.shape[1]))
    found = jnp.zeros((rows, ids.shape[1]), F32)
    for tile in range(tiles.shape[0] // rows):
        found = jnp.where(tile_of == tile + first, table[tile * rows : (tile + 1) * rows], found)
    return found


def spread(value, ids, iota, first, count):
    rows = value.shape[0]
    high, low = split(value)
    hot = one_hot(ids, iota)
    tile_of = jnp.broadcast_to(jnp.right_shift(ids, SHIFT), value.shape).astype(F32).astype(BF)
    zero = jnp.zeros_like(high)
    total = None
    for part in (high, low):
        left = jnp.concatenate(
            [jnp.where(tile_of == BF(tile + first), part, zero) for tile in range(count)], axis=0
        )
        term = lax.dot_general(left, hot, NT, preferred_element_type=F32)
        total = term if total is None else total + term
    return total


def face_kernel(source_ref, faces_ref, lower_ref, upper_ref, tiles, *, width):
    rows = source_ref.shape[0]
    fill_tiles(source_ref, tiles)
    iota = lax.broadcasted_iota(jnp.int32, (WIDE, width), 0)
    for side, out_ref in enumerate((lower_ref, upper_ref)):
        for start in range(0, faces_ref.shape[1], width):
            ids = faces_ref[side : side + 1, start : start + width]
            out_ref[:, start : start + width] = pick(tiles, ids, iota, rows, 0)


def curl_kernel(*refs, width, first, sources, added):
    source_refs = refs[:sources]
    ids_ref, curl_ref = refs[sources : sources + 2]
    prior_ref = refs[sources + 2] if added else None
    out_ref, tiles = refs[-2:]
    rows = source_refs[0].shape[0]
    start = 0
    for source_ref in source_refs:
        size = source_ref.shape[1] // WIDE * rows
        fill_tiles(source_ref, tiles.at[start : start + size])
        start += size
    blocks, nodes, length = ids_ref.shape
    steps = length // width
    iota = lax.broadcasted_iota(jnp.int32, (WIDE, width), 0)

    def body(step, carry):
        block = step // steps
        column = pl.multiple_of(step % steps * width, width)
        window = pl.ds(column, width)
        sums = [prior_ref[block, i, :, window] if added else None for i in range(3)]
        for j in range(nodes):
            found = pick(tiles, ids_ref[block, pl.ds(j, 1), window], iota, rows, first)
            for i in range(3):
                weight = jnp.broadcast_to(curl_ref[block, i, pl.ds(j, 1), window], found.shape)
                sums[i] = weight * found if sums[i] is None else sums[i] + weight * found
        for i in range(3):
            out_ref[block, i, :, window] = sums[i]
        return carry

    lax.fori_loop(0, blocks * steps, body, 0)


def curls(sources, ids, curl, first, prior=None):
    rows = sources[0].shape[0]
    blocks, nodes, length = ids.shape
    width = min(512, length)
    tiles = sum(s.shape[1] for s in sources) // WIDE
    extra = () if prior is None else (prior,)
    return pl.pallas_call(
        functools.partial(
            curl_kernel, width=width, first=first, sources=len(sources), added=prior is not None
        ),
        out_shape=jax.ShapeDtypeStruct((blocks, 3, rows, length), F32),
        in_specs=[VM] * (len(sources) + 2 + len(extra)),
        out_specs=VM,
        scratch_shapes=[pltpu.VMEM((tiles * rows, 2 * WIDE), BF)],
        cost_estimate=cost(tiles * rows * WIDE * 4 * blocks * nodes * length),
    )(*sources, ids, curl, *extra)


def assemble_kernel(field_ref, ids_ref, curl_ref, *refs, width, first, counts):
    out_refs, sums = refs[:-1], refs[-1]
    blocks, _, rows, length = field_ref.shape
    nodes = ids_ref.shape[1]
    steps = length // width
    count = sum(counts)
    sums[...] = jnp.zeros_like(sums)
    iota = lax.broadcasted_iota(jnp.int32, (WIDE, width), 0)

    def body(step, carry):
        block = step // steps
        column = pl.multiple_of(step % steps * width, width)
        window = pl.ds(column, width)
        field = [field_ref[block, i, :, window] for i in range(3)]
        total = None
        for j in range(nodes):
            value = None
            for i in range(3):
                weight = jnp.broadcast_to(curl_ref[block, i, pl.ds(j, 1), window], field[i].shape)
                value = weight * field[i] if value is None else value + weight * field[i]
            term = spread(value, ids_ref[block, pl.ds(j, 1), window], iota, first, count)
            total = term if total is None else total + term
        sums[...] += total
        return carry

    lax.fori_loop(0, blocks * steps, body, 0)
    tile = 0
    for out_ref, number in zip(out_refs, counts):
        for part in range(number):
            out_ref[:, part * WIDE : (part + 1) * WIDE] = sums[tile * rows : (tile + 1) * rows, :]
            tile += 1


def assemble(field, ids, curl, first, counts):
    blocks, _, rows, length = field.shape
    width = min(512, length)
    tiles = sum(counts)
    return pl.pallas_call(
        functools.partial(assemble_kernel, width=width, first=first, counts=counts),
        out_shape=[jax.ShapeDtypeStruct((rows, n * WIDE), F32) for n in counts],
        in_specs=[VM] * 3,
        out_specs=[VM] * len(counts),
        scratch_shapes=[pltpu.VMEM((tiles * rows, WIDE), F32)],
        cost_estimate=cost(tiles * rows * WIDE * 4 * blocks * ids.shape[1] * length),
    )(field, ids, curl)


def finish_kernel(own_ref, below_ref, above_ref, faces_ref, out_ref, *, width):
    rows, columns = own_ref.shape
    count = columns // WIDE
    iota = lax.broadcasted_iota(jnp.int32, (WIDE, width), 0)
    total = None
    for side, value_ref in enumerate((below_ref, above_ref)):
        for start in range(0, faces_ref.shape[1], width):
            window = slice(start, start + width)
            term = spread(value_ref[:, window], faces_ref[side : side + 1, window], iota, 0, count)
            total = term if total is None else total + term
    for tile in range(count):
        window = slice(tile * WIDE, (tile + 1) * WIDE)
        out_ref[:, window] = own_ref[:, window] + total[tile * rows : (tile + 1) * rows]


def curve_kernel(knots_ref, base_ref, slopes_ref, point_ref, nu_ref, twice_ref):
    samples, length = nu_ref.shape
    kinds = base_ref.shape[0]
    material = point_ref[3 * samples : 3 * samples + 1, :]
    masks = [material == float(kind) for kind in range(1, kinds)]

    def select(values):
        chosen = jnp.full((1, length), values[0], F32)
        for mask, value in zip(masks, values[1:]):
            chosen = jnp.where(mask, value, chosen)
        return chosen

    base = select([base_ref[kind] for kind in range(kinds)])
    knots = knots_ref.shape[0]
    slopes = [select([slopes_ref[kind, k] for kind in range(kinds)]) for k in range(knots)]
    starts = [knots_ref[k].astype(F32) * KNOT_STEP for k in range(knots)]

    def body(step, carry):
        row = pl.multiple_of(step * 8, 8)
        b = [point_ref[pl.ds(i * samples + row, 8), :] for i in range(3)]
        square = b[0] * b[0] + b[1] * b[1] + b[2] * b[2]
        nu = jnp.broadcast_to(base, square.shape)
        slope = jnp.zeros_like(square)
        for k in range(knots):
            z = (square - starts[k]) * (1.0 / KNOT_WIDTH)
            decay = jnp.exp(-jnp.abs(z))
            weight = jnp.broadcast_to(slopes[k], z.shape)
            nu = nu + weight * (jnp.maximum(z, 0.0) + jnp.log1p(decay))
            slope = slope + weight * (jnp.where(z >= 0.0, 1.0, decay) / (1.0 + decay))
        nu_ref[pl.ds(row, 8), :] = nu
        twice_ref[pl.ds(row, 8), :] = slope * (2.0 / KNOT_WIDTH)
        return carry

    lax.fori_loop(0, samples // 8, body, 0)


def tensor_kernel(flux_ref, point_ref, nu_ref, twice_ref, inverse_ref, forward_ref, out_ref):
    blocks, _, rows, length = flux_ref.shape
    samples = blocks * rows
    dot = functools.partial(
        jnp.dot, precision=lax.Precision.HIGHEST, preferred_element_type=F32
    )
    width = min(256, length)
    for start in range(0, length, width):
        window = slice(start, start + width)
        b = [point_ref[i * samples : (i + 1) * samples, window] for i in range(3)]
        flux = []
        for i in range(3):
            packed = jnp.concatenate([flux_ref[k, i, :, window] for k in range(blocks)], axis=0)
            flux.append(dot(inverse_ref[...], packed))
        along = b[0] * flux[0] + b[1] * flux[1] + b[2] * flux[2]
        along = along * twice_ref[:, window]
        nu = nu_ref[:, window]
        for i in range(3):
            coefs = dot(forward_ref[...], nu * flux[i] + along * b[i])
            for k in range(blocks):
                out_ref[k, i, :, window] = coefs[k * rows : (k + 1) * rows]


def per_device(
    field_in,
    faces,
    connectivity,
    curl_vectors,
    operating_point,
    material,
    bh_knots,
    curve_base,
    curve_slopes,
):
    rows, own = field_in.shape
    face_len = faces.shape[1]
    nodes, elements = connectivity.shape
    mesh_count = lax.axis_size("mesh")
    harm_count = lax.axis_size("harm")
    block = operating_point.shape[3]
    samples = operating_point.shape[0]
    length = elements // harm_count
    up = [(i, (i + 1) % mesh_count) for i in range(mesh_count)]
    down = [(j, i) for i, j in up]

    points = jnp.transpose(operating_point, (2, 1, 0, 3)).reshape(mesh_count, 3 * samples, block)
    kinds = jnp.broadcast_to(material.astype(F32)[:, None, :], (mesh_count, 8, block))
    points = jnp.concatenate([points, kinds], axis=1)
    points = lax.all_to_all(points, "mesh", split_axis=0, concat_axis=0, tiled=True)
    points = jnp.transpose(points, (1, 0, 2)).reshape(3 * samples + 8, length)

    ids = connectivity.reshape(nodes, mesh_count, harm_count, block)
    ids = jnp.transpose(ids, (2, 0, 1, 3)).reshape(harm_count, nodes, length)
    curl = curl_vectors.reshape(3, nodes, mesh_count, harm_count, block)
    curl = jnp.transpose(curl, (3, 0, 1, 2, 4)).reshape(harm_count, 3, nodes, length)

    face_width = min(512, face_len)
    own_tiles, face_tiles = own // WIDE, face_len // WIDE
    face_shape = jax.ShapeDtypeStruct((rows, face_len), F32)
    lower, upper = pl.pallas_call(
        functools.partial(face_kernel, width=face_width),
        out_shape=[face_shape, face_shape],
        in_specs=[VM] * 2,
        out_specs=[VM] * 2,
        scratch_shapes=[pltpu.VMEM((own_tiles * rows, 2 * WIDE), BF)],
        cost_estimate=cost(own * rows * 8 * face_len),
    )(field_in, faces)
    before = lax.ppermute(upper, "mesh", up)
    after = lax.ppermute(lower, "mesh", down)

    partial = curls([field_in], ids, curl, 0)
    flux = curls([before, after], ids, curl, own_tiles, partial)
    flux = lax.all_to_all(flux, "harm", split_axis=0, concat_axis=0, tiled=True)

    plane = jax.ShapeDtypeStruct((samples, length), F32)
    nu, twice = pl.pallas_call(
        curve_kernel,
        out_shape=[plane, plane],
        in_specs=[SM] * 3 + [VM],
        out_specs=[VM] * 2,
        cost_estimate=cost(samples * length * 8 * 40),
    )(bh_knots, curve_base, curve_slopes, points)

    inverse, forward = dft_tables(samples)
    field = pl.pallas_call(
        tensor_kernel,
        out_shape=jax.ShapeDtypeStruct(flux.shape, F32),
        in_specs=[VM] * 6,
        out_specs=VM,
        cost_estimate=cost(samples * samples * length * 6 * 12),
    )(flux, points, nu, twice, inverse, forward)
    field = lax.all_to_all(field, "harm", split_axis=0, concat_axis=0, tiled=True)

    low_sums, high_sums = assemble(field, ids, curl, own_tiles, (face_tiles, face_tiles))
    above = lax.ppermute(low_sums, "mesh", down)
    below = lax.ppermute(high_sums, "mesh", up)
    (own_sums,) = assemble(field, ids, curl, 0, (own_tiles,))
    return pl.pallas_call(
        functools.partial(finish_kernel, width=face_width),
        out_shape=jax.ShapeDtypeStruct((rows, own), F32),
        in_specs=[VM] * 4,
        out_specs=VM,
        cost_estimate=cost(own * rows * 8 * face_len),
    )(own_sums, below, above, faces)


def solution(mesh):
    return jax.shard_map(
        per_device,
        mesh=mesh,
        in_specs=(
            P("harm", "mesh"),
            P(None, "mesh"),
            P(None, "mesh"),
            P(None, None, "mesh"),
            P(None, None, None, ("mesh", "harm")),
            P(None, ("mesh", "harm")),
            P(),
            P(),
            P(),
        ),
        out_specs=P("harm", "mesh"),
        check_vma=False,
    )
```

```python
import functools

import jax
import jax.numpy as jnp
import numpy as np
from jax import lax
from jax.experimental import pallas as pl
from jax.experimental.pallas import tpu as pltpu
from jax.sharding import PartitionSpec as P

KNOT_STEP = 0.25
KNOT_WIDTH = 0.5
WIDE = 256
SHIFT = 8
BF = jnp.bfloat16
F32 = jnp.float32
VM = pl.BlockSpec(memory_space=pltpu.VMEM)
SM = pl.BlockSpec(memory_space=pltpu.SMEM)
NT = (((1,), (1,)), ((), ()))


def dft_tables(length):
    coef = np.arange(length)
    half = length // 2
    harmonic = np.where(coef < half, coef, coef - half + 1)
    harmonic = np.where(coef == length - 1, half, harmonic)
    is_sine = (coef >= half) & (coef < length - 1)
    angles = (harmonic[:, None] * coef[None, :] % length) * (2.0 * np.pi / length)
    rows = np.where(is_sine[:, None], np.sin(angles), np.cos(angles))
    weight = np.where((coef == 0) | (coef == length - 1), 1.0 / length, 2.0 / length)
    return rows.T.astype(np.float32), (rows * weight[:, None]).astype(np.float32)


def split(value):
    high = value.astype(BF)
    return high, (value - high.astype(F32)).astype(BF)


def cost(flops):
    return pl.CostEstimate(flops=flops, bytes_accessed=4 << 20, transcendentals=0)


def fill_tiles(source_ref, tiles):
    rows, columns = source_ref.shape
    for tile in range(columns // WIDE):
        high, low = split(source_ref[:, tile * WIDE : (tile + 1) * WIDE])
        tiles[tile * rows : (tile + 1) * rows, :WIDE] = high
        tiles[tile * rows : (tile + 1) * rows, WIDE:] = low


def one_hot(ids, iota):
    low = jnp.bitwise_and(ids, WIDE - 1)
    return (jnp.broadcast_to(low, iota.shape) == iota).astype(F32).astype(BF)


def pick(tiles, ids, iota, rows, first):
    hot = one_hot(ids, iota)
    table = jnp.dot(tiles[:, :WIDE], hot, preferred_element_type=F32)
    table = table + jnp.dot(tiles[:, WIDE:], hot, preferred_element_type=F32)
    tile_of = jnp.broadcast_to(jnp.right_shift(ids, SHIFT), (rows, ids.shape[1]))
    found = jnp.zeros((rows, ids.shape[1]), F32)
    for tile in range(tiles.shape[0] // rows):
        found = jnp.where(tile_of == tile + first, table[tile * rows : (tile + 1) * rows], found)
    return found


def spread(value, ids, iota, first, count):
    rows = value.shape[0]
    high, low = split(value)
    hot = one_hot(ids, iota)
    tile_of = jnp.broadcast_to(jnp.right_shift(ids, SHIFT), value.shape).astype(F32).astype(BF)
    zero = jnp.zeros_like(high)
    total = None
    for part in (high, low):
        left = jnp.concatenate(
            [jnp.where(tile_of == BF(tile + first), part, zero) for tile in range(count)], axis=0
        )
        term = lax.dot_general(left, hot, NT, preferred_element_type=F32)
        total = term if total is None else total + term
    return total


def face_kernel(source_ref, faces_ref, lower_ref, upper_ref, tiles, *, width):
    rows = source_ref.shape[0]
    fill_tiles(source_ref, tiles)
    iota = lax.broadcasted_iota(jnp.int32, (WIDE, width), 0)
    for side, out_ref in enumerate((lower_ref, upper_ref)):
        for start in range(0, faces_ref.shape[1], width):
            ids = faces_ref[side : side + 1, start : start + width]
            out_ref[:, start : start + width] = pick(tiles, ids, iota, rows, 0)


def element_rows(ref, index, chunk, width, block, span, owners):
    step = min(width, span)
    rows = []
    for part in range(width // step):
        place = chunk * width + part * step
        column = (place // span * owners + block) * span + place % span
        rows.append(ref[(*index, pl.ds(pl.multiple_of(column, step), step))])
    return rows[0] if len(rows) == 1 else jnp.concatenate(rows, axis=1)


def curl_kernel(block_ref, *refs, width, span, owners):
    source_refs, (ids_ref, curl_ref, out_ref, tiles) = refs[:-4], refs[-4:]
    rows = source_refs[0].shape[0]
    start = 0
    for source_ref in source_refs:
        size = source_ref.shape[1] // WIDE * rows
        fill_tiles(source_ref, tiles.at[start : start + size])
        start += size
    block = block_ref[0]
    nodes = ids_ref.shape[0]
    iota = lax.broadcasted_iota(jnp.int32, (WIDE, width), 0)

    def body(chunk, carry):
        take = functools.partial(
            element_rows, chunk=chunk, width=width, block=block, span=span, owners=owners
        )
        sums = [None] * 3
        for j in range(nodes):
            found = pick(tiles, take(ids_ref, (pl.ds(j, 1),)), iota, rows, 0)
            for i in range(3):
                weight = jnp.broadcast_to(take(curl_ref, (i, pl.ds(j, 1))), found.shape)
                sums[i] = weight * found if sums[i] is None else sums[i] + weight * found
        for i in range(3):
            out_ref[i, :, pl.ds(pl.multiple_of(chunk * width, width), width)] = sums[i]
        return carry

    lax.fori_loop(0, out_ref.shape[2] // width, body, 0)


def curls(block, sources, ids, curl, span, owners):
    rows = sources[0].shape[0]
    length = ids.shape[1] // owners
    width = min(512, length)
    tiles = sum(s.shape[1] for s in sources) // WIDE
    return pl.pallas_call(
        functools.partial(curl_kernel, width=width, span=span, owners=owners),
        out_shape=jax.ShapeDtypeStruct((3, rows, length), F32),
        in_specs=[SM] + [VM] * (len(sources) + 2),
        out_specs=VM,
        scratch_shapes=[pltpu.VMEM((tiles * rows, 2 * WIDE), BF)],
        cost_estimate=cost(tiles * rows * WIDE * 4 * ids.shape[0] * length),
    )(block, *sources, ids, curl)


def assemble_kernel(block_ref, field_ref, ids_ref, curl_ref, *refs, width, span, owners, first, counts, added):
    prior_ref = refs[0] if added else None
    out_refs, sums = refs[1 if added else 0 : -1], refs[-1]
    _, rows, length = field_ref.shape
    block = block_ref[0]
    nodes = ids_ref.shape[0]
    count = sums.shape[0] // rows
    sums[...] = prior_ref[first * rows : (first + count) * rows, :] if added else jnp.zeros_like(sums)
    iota = lax.broadcasted_iota(jnp.int32, (WIDE, width), 0)

    def body(chunk, carry):
        take = functools.partial(
            element_rows, chunk=chunk, width=width, block=block, span=span, owners=owners
        )
        window = pl.ds(pl.multiple_of(chunk * width, width), width)
        field = [field_ref[i, :, window] for i in range(3)]
        total = None
        for j in range(nodes):
            value = None
            for i in range(3):
                weight = jnp.broadcast_to(take(curl_ref, (i, pl.ds(j, 1))), field[i].shape)
                value = weight * field[i] if value is None else value + weight * field[i]
            term = spread(value, take(ids_ref, (pl.ds(j, 1),)), iota, first, count)
            total = term if total is None else total + term
        sums[...] += total
        return carry

    lax.fori_loop(0, length // width, body, 0)
    if counts is None:
        out_refs[0][...] = sums[...]
        return
    tile = 0
    for out_ref, number in zip(out_refs, counts):
        for part in range(number):
            out_ref[:, part * WIDE : (part + 1) * WIDE] = sums[tile * rows : (tile + 1) * rows, :]
            tile += 1


def assemble(block, field, ids, curl, span, owners, prior, first, count, counts=None):
    _, rows, length = field.shape
    width = min(512, length)
    extra = () if prior is None else (prior,)
    if counts is None:
        out_shape = [jax.ShapeDtypeStruct((count * rows, WIDE), F32)]
    else:
        out_shape = [jax.ShapeDtypeStruct((rows, n * WIDE), F32) for n in counts]
    return pl.pallas_call(
        functools.partial(
            assemble_kernel, width=width, span=span, owners=owners, first=first, counts=counts,
            added=prior is not None,
        ),
        out_shape=out_shape,
        in_specs=[SM] + [VM] * (3 + len(extra)),
        out_specs=[VM] * len(out_shape),
        scratch_shapes=[pltpu.VMEM((count * rows, WIDE), F32)],
        cost_estimate=cost(count * rows * WIDE * 4 * ids.shape[0] * length),
    )(block, field, ids, curl, *extra)


def finish_kernel(own_ref, below_ref, above_ref, faces_ref, out_ref, *, width):
    rows, columns = own_ref.shape
    count = columns // WIDE
    iota = lax.broadcasted_iota(jnp.int32, (WIDE, width), 0)
    total = None
    for side, value_ref in enumerate((below_ref, above_ref)):
        for start in range(0, faces_ref.shape[1], width):
            window = slice(start, start + width)
            term = spread(value_ref[:, window], faces_ref[side : side + 1, window], iota, 0, count)
            total = term if total is None else total + term
    for tile in range(count):
        window = slice(tile * WIDE, (tile + 1) * WIDE)
        out_ref[:, window] = own_ref[:, window] + total[tile * rows : (tile + 1) * rows]


def curve_kernel(knots_ref, base_ref, slopes_ref, point_ref, nu_ref, twice_ref):
    samples, length = nu_ref.shape
    kinds = base_ref.shape[0]
    material = point_ref[3 * samples : 3 * samples + 1, :]
    masks = [material == float(kind) for kind in range(1, kinds)]

    def select(values):
        chosen = jnp.full((1, length), values[0], F32)
        for mask, value in zip(masks, values[1:]):
            chosen = jnp.where(mask, value, chosen)
        return chosen

    base = select([base_ref[kind] for kind in range(kinds)])
    knots = knots_ref.shape[0]
    slopes = [select([slopes_ref[kind, k] for kind in range(kinds)]) for k in range(knots)]
    starts = [knots_ref[k].astype(F32) * KNOT_STEP for k in range(knots)]

    def body(step, carry):
        row = pl.multiple_of(step * 8, 8)
        b = [point_ref[pl.ds(i * samples + row, 8), :] for i in range(3)]
        square = b[0] * b[0] + b[1] * b[1] + b[2] * b[2]
        nu = jnp.broadcast_to(base, square.shape)
        slope = jnp.zeros_like(square)
        for k in range(knots):
            z = (square - starts[k]) * (1.0 / KNOT_WIDTH)
            decay = jnp.exp(-jnp.abs(z))
            weight = jnp.broadcast_to(slopes[k], z.shape)
            nu = nu + weight * (jnp.maximum(z, 0.0) + jnp.log1p(decay))
            slope = slope + weight * (jnp.where(z >= 0.0, 1.0, decay) / (1.0 + decay))
        nu_ref[pl.ds(row, 8), :] = nu
        twice_ref[pl.ds(row, 8), :] = slope * (2.0 / KNOT_WIDTH)
        return carry

    lax.fori_loop(0, samples // 8, body, 0)


def tensor_kernel(me_ref, *refs):
    blocks = (len(refs) - 5) // 2
    flux_refs, out_refs = refs[:blocks], refs[blocks + 5 :]
    point_ref, nu_ref, twice_ref, inverse_ref, forward_ref = refs[blocks : blocks + 5]
    _, rows, length = flux_refs[0].shape
    samples = blocks * rows
    me = me_ref[0]
    inverse, forward = inverse_ref[me], forward_ref[me]
    dot = functools.partial(
        jnp.dot, precision=lax.Precision.HIGHEST, preferred_element_type=F32
    )
    width = min(256, length)
    for start in range(0, length, width):
        window = slice(start, start + width)
        b = [point_ref[i * samples : (i + 1) * samples, window] for i in range(3)]
        flux = []
        for i in range(3):
            packed = jnp.concatenate([ref[i, :, window] for ref in flux_refs], axis=0)
            flux.append(dot(inverse, packed))
        along = b[0] * flux[0] + b[1] * flux[1] + b[2] * flux[2]
        along = along * twice_ref[:, window]
        nu = nu_ref[:, window]
        for i in range(3):
            coefs = dot(forward, nu * flux[i] + along * b[i])
            for k, ref in enumerate(out_refs):
                ref[i, :, window] = coefs[k * rows : (k + 1) * rows]


def ordered_tables(samples, owners):
    inverse, forward = dft_tables(samples)
    rows = samples // owners
    inverse = inverse.reshape(samples, owners, rows)
    forward = forward.reshape(owners, rows, samples)
    arrival = [[(me - k) % owners for k in range(owners)] for me in range(owners)]
    sending = [[(me + k) % owners for k in range(owners)] for me in range(owners)]
    return (
        np.stack([inverse[:, o].reshape(samples, samples) for o in arrival]),
        np.stack([forward[o].reshape(samples, samples) for o in sending]),
    )


def per_device(
    field_in,
    faces,
    connectivity,
    curl_vectors,
    operating_point,
    material,
    bh_knots,
    curve_base,
    curve_slopes,
):
    rows, own = field_in.shape
    face_len = faces.shape[1]
    nodes, elements = connectivity.shape
    mesh_count = lax.axis_size("mesh")
    harm_count = lax.axis_size("harm")
    block = operating_point.shape[3]
    samples = operating_point.shape[0]
    length = elements // harm_count
    up = [(i, (i + 1) % mesh_count) for i in range(mesh_count)]
    down = [(j, i) for i, j in up]

    points = jnp.transpose(operating_point, (2, 1, 0, 3)).reshape(mesh_count, 3 * samples, block)
    kinds = jnp.broadcast_to(material.astype(F32)[:, None, :], (mesh_count, 8, block))
    points = jnp.concatenate([points, kinds], axis=1)
    points = lax.all_to_all(points, "mesh", split_axis=0, concat_axis=0, tiled=True)
    points = jnp.transpose(points, (1, 0, 2)).reshape(3 * samples + 8, length)

    ids, curl, span = connectivity, curl_vectors, block
    if block % 128:
        span = length
        ids = ids.reshape(nodes, mesh_count, harm_count, block)
        ids = jnp.transpose(ids, (0, 2, 1, 3)).reshape(nodes, elements)
        curl = curl.reshape(3, nodes, mesh_count, harm_count, block)
        curl = jnp.transpose(curl, (0, 1, 3, 2, 4)).reshape(3, nodes, elements)
    me = lax.axis_index("harm")
    at = [jnp.reshape((me + k) % harm_count, (1,)) for k in range(harm_count)]
    order = sorted(range(1, harm_count), key=lambda k: (-min(k, harm_count - k), k))

    def send(value, k):
        return lax.ppermute(value, "harm", [(i, (i + k) % harm_count) for i in range(harm_count)])

    face_width = min(512, face_len)
    own_tiles, face_tiles = own // WIDE, face_len // WIDE
    face_shape = jax.ShapeDtypeStruct((rows, face_len), F32)
    lower, upper = pl.pallas_call(
        functools.partial(face_kernel, width=face_width),
        out_shape=[face_shape, face_shape],
        in_specs=[VM] * 2,
        out_specs=[VM] * 2,
        scratch_shapes=[pltpu.VMEM((own_tiles * rows, 2 * WIDE), BF)],
        cost_estimate=cost(own * rows * 8 * face_len),
    )(field_in, faces)
    before = lax.ppermute(upper, "mesh", up)
    after = lax.ppermute(lower, "mesh", down)

    flux = {}
    for k in order + [0]:
        piece = curls(at[k], [field_in, before, after], ids, curl, span, harm_count)
        flux[k] = send(piece, k) if k else piece

    plane = jax.ShapeDtypeStruct((samples, length), F32)
    nu, twice = pl.pallas_call(
        curve_kernel,
        out_shape=[plane, plane],
        in_specs=[SM] * 3 + [VM],
        out_specs=[VM] * 2,
        cost_estimate=cost(samples * length * 8 * 40),
    )(bh_knots, curve_base, curve_slopes, points)

    inverse, forward = ordered_tables(samples, harm_count)
    piece = jax.ShapeDtypeStruct((3, rows, length), F32)
    fields = pl.pallas_call(
        tensor_kernel,
        out_shape=[piece] * harm_count,
        in_specs=[SM] + [VM] * (harm_count + 5),
        out_specs=[VM] * harm_count,
        cost_estimate=cost(samples * samples * length * 6 * 12),
    )(at[0], *(flux[k] for k in range(harm_count)), points, nu, twice, inverse, forward)

    back = order[::-1]
    field = {k: send(fields[k], k) for k in back}
    field[0] = fields[0]
    put = functools.partial(assemble, ids=ids, curl=curl, span=span, owners=harm_count)
    tiles = own_tiles + 2 * face_tiles
    sums = None
    for k in [0] + back[:-1]:
        (sums,) = put(at[-k % harm_count], field[k], prior=sums, first=0, count=tiles)
    last = back[-1]
    where = at[-last % harm_count]
    low_sums, high_sums = put(
        where, field[last], prior=sums, first=own_tiles, count=2 * face_tiles,
        counts=(face_tiles, face_tiles),
    )
    above = lax.ppermute(low_sums, "mesh", down)
    below = lax.ppermute(high_sums, "mesh", up)
    (own_sums,) = put(
        where, field[last], prior=sums, first=0, count=own_tiles, counts=(own_tiles,)
    )
    return pl.pallas_call(
        functools.partial(finish_kernel, width=face_width),
        out_shape=jax.ShapeDtypeStruct((rows, own), F32),
        in_specs=[VM] * 4,
        out_specs=VM,
        cost_estimate=cost(own * rows * 8 * face_len),
    )(own_sums, below, above, faces)


def solution(mesh):
    return jax.shard_map(
        per_device,
        mesh=mesh,
        in_specs=(
            P("harm", "mesh"),
            P(None, "mesh"),
            P(None, "mesh"),
            P(None, None, "mesh"),
            P(None, None, None, ("mesh", "harm")),
            P(None, ("mesh", "harm")),
            P(),
            P(),
            P(),
        ),
        out_specs=P("harm", "mesh"),
        check_vma=False,
    )
```
